256 devices in a mesh: grp: 4 (over y, x), seq: 64 (over z, core).
Axes of the slice: x: 2, y: 2, z: 32, core: 2. Of those that a mesh axis runs over, the one named last changes fastest.
The devices are a block of a 4x8x32 slice.
Arguments:
- corpus: bfloat16 [65536, 3584], P(('grp', 'seq')), parts along dimension 0, may hold values from -6 to 6
- window_ends: int32 [512], P(('grp', 'seq')), parts along dimension 0, may hold values from 0 to 255
- norm_gain: float32 [3584], replicated, may hold values from 0.5 to 1.5
- routes: int32 [8192, 2], P(('grp', 'seq')), parts along dimension 0, may hold values from 0 to 63, all different within a row; in each aligned block of 32 rows (0 to 31, 32 to 63, ...) at most 2 rows name the same one
- in_blocks: int32 [64, 7], replicated, may hold values from 0 to 27, all different within a row
- out_blocks: int32 [64, 7], replicated, may hold values from 0 to 27, all different within a row
- enc_weight: bfloat16 [896, 131072], P(None, 'seq'), may hold values from -0.1875 to 0.1875
- enc_bias: float32 [131072], P('seq'), may hold values from -3 to 3
- latent_cutoffs: float32 [131072], P('seq'), may hold values from 0.2 to 1.2
- dec_weight: bfloat16 [131072, 896], P('seq'), may hold values from -0.125 to 0.125
- readout: float32 [131072], P('seq'), may hold values from -1.5 to 1.5
- dec_bias: float32 [3584], replicated, may hold values from -3 to 3
Outputs:
- reconstruction: bfloat16 [65536, 3584], P(('grp', 'seq')), parts along dimension 0
- attribution: bfloat16 [65536, 3584], P(('grp', 'seq')), parts along dimension 0
- feature_score: float32 [65536], P(('grp', 'seq')), parts along dimension 0
The draws below stay inside these ranges and needn't reach their ends.
There are 4 independent parts, one for each index of `grp`. The reference program is written for one: setup_inputs(seed, part) draws one part's arguments, and reference() takes and returns one part's arrays. A program takes and returns all parts, laid end to end along the dimension named above; an argument that names none is the same for every part. Nothing has to cross between parts.
Inputs may be any that keep to these rules, and one draw needn't show every extreme that they name: `routes`: each segment names 2 different feature groups; within the 32 segments of one device no group is named more than 2 times. `in_blocks`: each row names 7 different blocks, and every block is named by some row. `out_blocks`: each row names 7 different blocks, and every block is named by some row.
All inputs are finite; a program needn't handle non-finite values.
Results may differ from the reference program's by a relative error of at most 0.012.
Values may be sent and summed in bfloat16 or wider, within the bound.
A program may use at most 128 MiB of HBM per device.

```python
import math
import jax
import jax.numpy as jnp
import numpy as np
from jax import lax

D = 3584
BLK = 128
KEEP = 7
FEAT_DEV = 2048
LEN = 128
SEG = 8
TOPK = 2
WIN_DEV = 2
DBLK = 28
CORP_DEV = 256
SEGS = 32
CAP = 2
FEATURES = 131072
WINDOWS = 128
TOKENS = 16384
CORPUS = 16384
SEGMENTS = 2048
N_SEQ = 64


def plant(entries, rng, smallest, high):
    index_at = [jax.random.randint(jax.random.fold_in(rng, axis), (), 0, length) for axis, length in enumerate(entries.shape)]
    widest = entries.shape.index(max(entries.shape))
    neighbour = index_at[:widest] + [(index_at[widest] + 1) % entries.shape[widest]] + index_at[widest + 1:]
    return entries.at[tuple(index_at)].set(smallest).at[tuple(neighbour)].set(high)


def block_levels(own_key, extent, pieces, low, top_value):
    def one(position, parts):
        draws = jax.random.uniform(jax.random.fold_in(jax.random.fold_in(own_key, 6), position), (parts,), jnp.float32, low / len(pieces), top_value / len(pieces))
        return jnp.repeat(jnp.exp(draws), extent[position] // parts).reshape((-1,) + (1,) * (len(extent) - position - 1))

    factor_of = one(*pieces[0])
    for cut in pieces[1:]:
        factor_of = factor_of * one(*cut)
    return factor_of


def picks_of(own_key, rows, count, top, lift):
    order = jax.random.permutation(jax.random.fold_in(own_key, 1), count)
    pull = order
    for power in range(3):
        pull = pull * pull // count
    pull = pull * lift // count
    chance = jax.random.randint(jax.random.fold_in(own_key, 2), (rows, count), 0, 4096) + pull
    holders = jax.random.permutation(jax.random.fold_in(own_key, 3), rows)[jnp.arange(count) % rows]
    chance = jnp.where(jnp.arange(rows)[:, None] == holders[None, :], 1 << 14, chance)
    merit = chance * count + jnp.arange(count)
    return lax.top_k(merit.astype(jnp.int32), top)[1].astype(jnp.int32)


def shared_out(key, own, number, rows, count, top, limit, slope):
    sequence = jax.random.permutation(key, count)
    crowded, ordinary = load_shares(count, rows * top, limit, slope, True), load_shares(count, rows * top, limit, slope, False)
    places = jnp.arange(count)

    def named(tallies, rotation):
        used = int((tallies > 0).sum())
        fixed = max(1, used // 4)
        shifted = fixed + (places - fixed + rotation * (used - fixed)) % max(1, count - fixed)
        return jnp.zeros((count,), jnp.int32).at[sequence[jnp.where(places < fixed, places, shifted)]].set(jnp.asarray(tallies, jnp.int32))

    tallies = jnp.where(number % 4 == 0, named(crowded, number // 4), named(ordinary, number - number // 4 - 1))
    mixed = jax.random.permutation(jax.random.fold_in(own, 3), count)
    source_of, taker = mixed[0:count // 2 * 2:2], mixed[1:count // 2 * 2:2]
    margin = jnp.minimum(tallies[source_of] - 1, limit - tallies[taker]) // 2
    margin = jnp.where((source_of == sequence[0]) | (taker == sequence[0]) | (tallies[taker] == 0), 0, jnp.maximum(margin, 0))
    shifted = jax.random.randint(jax.random.fold_in(own, 4), (count // 2,), 0, 1 << 20) % (margin + 1)
    tallies = tallies.at[source_of].add(-shifted).at[taker].add(shifted)
    items = jnp.searchsorted(jnp.cumsum(tallies), jnp.arange(rows * top), side="right").astype(jnp.int32)
    table = items.reshape(top, rows).T
    table = table[jax.random.permutation(jax.random.fold_in(own, 1), rows)]
    rotation = jax.random.randint(jax.random.fold_in(own, 2), (rows, 1), 0, top)
    return jnp.take_along_axis(table, (jnp.arange(top)[None, :] + rotation) % top, axis=1)


def load_shares(number_of, total, limit, lean, full):
    weights = [(1 << 20) // math.isqrt(grade ** lean) + 1 for grade in range(1, number_of + 1)]
    largest = limit if full else min(limit, max(-(-total // number_of), total * weights[0] // sum(weights)))
    least = 1 if total - largest >= number_of - 1 else 0
    counts, spare = [largest] + [least] * (number_of - 1), total - largest - least * (number_of - 1)
    while spare > 0:
        candidates = [i for i in range(1, number_of) if counts[i] < largest] or [i for i in range(1, number_of) if counts[i] < limit]
        whole, left = sum([weights[i] for i in candidates]), spare
        for i in candidates:
            addition = min(limit - counts[i], max(1, left * weights[i] // whole), spare)
            counts[i] = counts[i] + addition
            spare = spare - addition
    return np.array(counts)


def bell_draw(key, extent, width, reach, cuts=(), kind=jnp.bfloat16):
    array = width * jax.random.normal(key, extent, jnp.float32)
    if cuts:
        array = array * block_levels(key, extent, cuts, -0.22, 0.18)
    return jnp.clip(array, -reach, reach).astype(kind)


def setup_inputs(seed: int = 0, part: int = 0) -> dict:
    streams_of = jax.random.split(jax.random.key(seed), 13)
    part_keys = jax.random.split(jax.random.fold_in(streams_of[12], part), 13)
    corpus = bell_draw(part_keys[0], (CORPUS, D), 1.0, 6.0, ((0, 64),))
    window_ends = plant(jax.random.randint(part_keys[1], (WINDOWS,), 0, CORP_DEV), jax.random.fold_in(part_keys[1], 1), 0, CORP_DEV - 1).astype(jnp.int32)
    norm_gain = jnp.clip(1.0 + 0.1 * jax.random.normal(streams_of[2], (D,), jnp.float32), 0.5, 1.5)
    routes_keys = jax.random.split(jax.random.fold_in(part_keys[3], 1), SEGMENTS // SEGS)
    routes_turns = jax.random.permutation(jax.random.fold_in(part_keys[3], 3), SEGMENTS // SEGS)
    routes = jax.vmap(lambda own, number: shared_out(jax.random.fold_in(part_keys[3], 2), own, number, SEGS, N_SEQ, TOPK, CAP, 2))(routes_keys, routes_turns).reshape((SEGMENTS, TOPK))
    in_blocks = picks_of(streams_of[4], N_SEQ, D // BLK, KEEP, 0)
    out_blocks = picks_of(streams_of[5], N_SEQ, D // BLK, KEEP, 0)
    enc_weight = bell_draw(streams_of[6], (KEEP * BLK, FEATURES), (KEEP * BLK) ** -0.5, 0.1875, ((1, 64),))
    enc_bias = bell_draw(streams_of[7], (FEATURES,), 0.5, 3.0, ((0, 64),), jnp.float32)
    latent_cutoffs = jnp.clip(jnp.exp(math.log(1.2) - 1.7917595 * jax.random.uniform(streams_of[8], (FEATURES,), jnp.float32) ** block_levels(streams_of[8], (FEATURES,), ((0, 64),), -0.2, 0.2)), 0.2, 1.2)
    dec_weight = bell_draw(streams_of[9], (FEATURES, KEEP * BLK), FEAT_DEV ** -0.5, 0.125, ((0, 64),))
    readout = bell_draw(streams_of[10], (FEATURES,), 0.25, 1.5, ((0, 64),), jnp.float32)
    dec_bias = bell_draw(streams_of[11], (D,), 0.5, 3.0, (), jnp.float32)
    return dict(corpus=corpus, window_ends=window_ends, norm_gain=norm_gain, routes=routes, in_blocks=in_blocks, out_blocks=out_blocks, enc_weight=enc_weight, enc_bias=enc_bias, latent_cutoffs=latent_cutoffs, dec_weight=dec_weight, readout=readout, dec_bias=dec_bias)


step_sharpness = 0.1
norm_eps = 1e-06

def normalize(rows, norm_gain):
    widened = rows.astype(jnp.float32)
    inverse_rms = lax.rsqrt(lax.optimization_barrier(jnp.mean(widened * widened, axis=-1, keepdims=True)) + norm_eps)
    return (widened * inverse_rms * norm_gain).astype(jnp.bfloat16)

def window_rows(corpus, window_ends):
    padded = jnp.concatenate([jnp.zeros((LEN, D), corpus.dtype), corpus], axis=0)
    owners = jnp.arange(WINDOWS, dtype=jnp.int32) // WIN_DEV * CORP_DEV
    starts = (owners + window_ends + 1).astype(jnp.int32)

    def take_one(start):
        return lax.dynamic_slice_in_dim(padded, start, LEN, 0)
    return jax.vmap(take_one)(starts).reshape(WINDOWS * LEN, D)

def group_terms(segment, group_id, in_blocks, out_blocks, enc_weight, enc_bias, latent_cutoffs, dec_weight, readout):
    input_ids = in_blocks[group_id]
    output_ids = out_blocks[group_id]
    first = (group_id * FEAT_DEV).astype(jnp.int32)
    blocks = segment.reshape(SEG, DBLK, BLK)
    chosen = jnp.take(blocks, input_ids, axis=1).reshape(SEG, KEEP * BLK)
    enc_slice = lax.dynamic_slice_in_dim(enc_weight, first, FEAT_DEV, 1)
    dec_slice = lax.dynamic_slice_in_dim(dec_weight, first, FEAT_DEV, 0)
    bias_slice = lax.dynamic_slice_in_dim(enc_bias, first, FEAT_DEV, 0)
    cutoff_contribution = lax.dynamic_slice_in_dim(latent_cutoffs, first, FEAT_DEV, 0)
    output_contribution = lax.dynamic_slice_in_dim(readout, first, FEAT_DEV, 0)
    latent_input_level = jnp.dot(chosen, enc_slice, preferred_element_type=jnp.float32) + bias_slice
    exceeds_cutoff_indicator = jax.nn.sigmoid((latent_input_level - cutoff_contribution) / step_sharpness)
    nonzero_latent_count = latent_input_level * exceeds_cutoff_indicator
    active_half = nonzero_latent_count.astype(jnp.bfloat16)
    decoded = jnp.dot(active_half, dec_slice, preferred_element_type=jnp.float32).astype(jnp.bfloat16)
    score_term = lax.optimization_barrier(jnp.sum(nonzero_latent_count * output_contribution, axis=-1)).astype(jnp.bfloat16)
    midpoint_gradient = (output_contribution * (exceeds_cutoff_indicator + latent_input_level * exceeds_cutoff_indicator * (1.0 - exceeds_cutoff_indicator) / step_sharpness)).astype(jnp.bfloat16)
    pulled = jnp.dot(midpoint_gradient, enc_slice.T, preferred_element_type=jnp.float32).astype(jnp.bfloat16)
    placed_out = jnp.zeros((SEG, DBLK, BLK), jnp.float32).at[:, output_ids].set(decoded.astype(jnp.float32).reshape(SEG, KEEP, BLK))
    placed_in = jnp.zeros((SEG, DBLK, BLK), jnp.float32).at[:, input_ids].set(pulled.astype(jnp.float32).reshape(SEG, KEEP, BLK))
    return (placed_out.reshape(SEG, D), placed_in.reshape(SEG, D), score_term.astype(jnp.float32))

def reference(corpus, window_ends, norm_gain, routes, in_blocks, out_blocks, enc_weight, enc_bias, latent_cutoffs, dec_weight, readout, dec_bias):
    normal = normalize(window_rows(corpus, window_ends), norm_gain)
    segments = normal.reshape(SEGMENTS, SEG, D)

    def per_segment(packed):
        segment, route_row = packed
        recon_sum = jnp.zeros((SEG, D), jnp.float32)
        grad_sum = jnp.zeros((SEG, D), jnp.float32)
        score_sum = jnp.zeros((SEG,), jnp.float32)
        for route_slot in range(TOPK):
            decoded, pulled, score_term = group_terms(segment, route_row[route_slot], in_blocks, out_blocks, enc_weight, enc_bias, latent_cutoffs, dec_weight, readout)
            recon_sum = recon_sum + decoded
            grad_sum = grad_sum + pulled
            score_sum = score_sum + score_term
        return (recon_sum, grad_sum, score_sum)
    recon_sum, grad_sum, score_sum = lax.map(per_segment, (segments, routes))
    reconstruction = (recon_sum.reshape(TOKENS, D) + dec_bias).astype(jnp.bfloat16)
    attribution = (normal.astype(jnp.float32) * grad_sum.reshape(TOKENS, D)).astype(jnp.bfloat16)
    return (reconstruction, attribution, score_sum.reshape(TOKENS))
```

```python
import functools
import itertools

import jax
import jax.numpy as jnp
from jax import lax
from jax.experimental import pallas as pl
from jax.experimental.pallas import tpu as pltpu
from jax.sharding import PartitionSpec as P

BLK = 128
KEEP = 7
LEN = 128
SEG = 8
CAP = 2
CORES = 2
PIECES = 4

step_sharpness = 0.1
norm_eps = 1e-06

USUAL = (38, 36, 34, 31, 29, 27, 25, 24, 22, 20, 17, 15, 13, 11, 8, 5)


def most(hops):
    return tuple(CORES * CAP * (hops + 1 - t) for t in range(1, hops + 1))


def starts_of(limits):
    return tuple(itertools.accumulate((0,) + limits[:-1]))


def pieces_of(limits):
    size = -(-limits[0] // PIECES)
    pieces = [[(a, min(a + size, count)) for a in range(0, count, size)] for count in limits]
    firsts = starts_of(tuple(len(cut) for cut in pieces))
    return pieces, firsts, firsts[-1] + len(pieces[-1])


def ways(me, devices):
    return ((me + CORES) % devices, (me + devices - CORES) % devices)


def meet(others):
    barrier = pltpu.get_barrier_semaphore()
    for other in others:
        pl.semaphore_signal(
            barrier, inc=1, device_id={"seq": other}, device_id_type=pl.DeviceIdType.MESH
        )
    pl.semaphore_wait(barrier, len(others))


def to(other, src, dst, send_sem, recv_sem):
    return pltpu.make_async_remote_copy(
        src_ref=src,
        dst_ref=dst,
        send_sem=send_sem,
        recv_sem=recv_sem,
        device_id={"seq": other},
        device_id_type=pl.DeviceIdType.MESH,
    )


def carry_kernel(
    limits, devices, items, notes, x, heard, heard_near, lists, stage, known,
    s_data, r_data, s_note, r_note, s_near, r_near, s_last, r_last, read_sem,
):
    hops = len(limits)
    first = limits[0]
    pieces, firsts, _ = pieces_of(limits)
    slots = 4 * hops + 2
    me = lax.axis_index("seq")
    mate = me + 1 - 2 * (me % 2)
    onward = ways(me, devices)
    meet((*onward, mate))
    started = []

    def send(t, way, q, a, b):
        src = items.at[pl.ds(way * first + a, b - a)] if t == 1 else (
            lists[way][t - 2].at[pl.ds(a, b - a)]
        )
        copy = to(
            onward[way], src, lists[way][t - 1].at[pl.ds(a, b - a)],
            s_data.at[way, firsts[t - 1] + q], r_data.at[way, firsts[t - 1] + q],
        )
        copy.start()
        started.append(copy)
        return copy

    def send_note(t, way):
        src = notes.at[way] if t == 1 else heard.at[way, t - 2]
        copy = to(
            onward[way], src, heard.at[way, t - 1], s_note.at[way, t - 1], r_note.at[way, t - 1]
        )
        copy.start()
        started.append(copy)
        return copy

    note_copies = {}
    data_copies = {}
    for way in (0, 1):
        note_copies[1, way] = send_note(1, way)
    for q, (a, b) in enumerate(pieces[0]):
        for way in (0, 1):
            data_copies[1, way, q] = send(1, way, q, a, b)
    local = 2 * first
    near = to(
        mate, items.at[pl.ds(local + CAP, CAP)], x.at[pl.ds(slots + 4 * hops, CAP)],
        s_last.at[0], r_last.at[0],
    )
    near.start()
    near_note = to(mate, notes, heard_near.at[:, 0], s_last.at[1], r_last.at[1])
    near_note.start()
    mate_copies = [near, near_note]
    for j in range(CAP):
        x[4 * hops + j] = items[local + j]

    def hand_over(k, lo, hi):
        copy = to(
            mate, stage.at[pl.ds(4 * lo, 4 * (hi - lo))], x.at[pl.ds(slots + 4 * lo, 4 * (hi - lo))],
            s_near.at[k], r_near.at[k],
        )
        copy.start()
        mate_copies.append(copy)

    handed = 0
    batch = 4
    for t in range(1, hops + 1):
        reads = []
        for way in (0, 1):
            note_copies[t, way].wait_recv()
            if t < hops:
                note_copies[t + 1, way] = send_note(t + 1, way)
            reads.append(pltpu.make_async_copy(
                heard.at[way, t - 1], known.at[way, t - 1], read_sem.at[way, t - 1]
            ))
            reads[-1].start()
        following = pieces[t] if t < hops else []
        for q, _ in enumerate(pieces[t - 1]):
            for way in (0, 1):
                data_copies[t, way, q].wait_recv()
                if q < len(following):
                    data_copies[t + 1, way, q] = send(t + 1, way, q, *following[q])
        if t > 1 and (t - 1) % batch == 0:
            hand_over((t - 1) // batch - 1, handed, t - 1)
            handed = t - 1
        for read in reads:
            read.wait()
        for way in (0, 1):
            for j in range(CAP):
                slot = 4 * (t - 1) + CAP * way + j
                for who, out in ((me, x), (mate, stage)):
                    place = jnp.clip(known[way, t - 1, 0, j * devices + who], 0, limits[t - 1] - 1)
                    out[slot] = lists[way][t - 1][place]
    hand_over((hops - 1) // batch, handed, hops)
    relay = to(mate, heard, heard_near.at[:, pl.ds(1, hops)], s_last.at[2], r_last.at[2])
    relay.start()
    mate_copies.append(relay)
    for copy in mate_copies:
        copy.wait_recv()
    for copy in started + mate_copies:
        copy.wait_send()


def carry(limits, devices, items, notes, collective_id):
    hops = len(limits)
    slots = 4 * hops + 2
    piece_count = pieces_of(limits)[2]
    shape = items.shape[1:]
    batches = (hops - 1) // 4 + 1
    vmem = pl.BlockSpec(memory_space=pltpu.VMEM)
    smem = pl.BlockSpec(memory_space=pltpu.SMEM)
    dma = pltpu.SemaphoreType.DMA
    return pl.pallas_call(
        functools.partial(carry_kernel, limits, devices),
        out_shape=(
            jax.ShapeDtypeStruct((2 * slots, *shape), items.dtype),
            jax.ShapeDtypeStruct((2, hops, 1, notes.shape[-1]), jnp.int32),
            jax.ShapeDtypeStruct((2, hops + 1, 1, notes.shape[-1]), jnp.int32),
        ),
        in_specs=[vmem, vmem],
        out_specs=(vmem, vmem, vmem),
        scratch_shapes=[
            [[pltpu.VMEM((limit, *shape), items.dtype) for limit in limits] for _ in (0, 1)],
            pltpu.VMEM((4 * hops, *shape), items.dtype),
            pltpu.SMEM((2, hops, 1, notes.shape[-1]), jnp.int32),
            dma((2, piece_count)),
            dma((2, piece_count)),
            dma((2, hops)),
            dma((2, hops)),
            dma((batches,)),
            dma((batches,)),
            dma((3,)),
            dma((3,)),
            dma((2, hops)),
        ],
        compiler_params=pltpu.CompilerParams(
            collective_id=collective_id, has_side_effects=True, vmem_limit_bytes=60 << 20
        ),
        name=f"carry{collective_id}",
    )(items, notes)


def bring_kernel(
    limits, devices, y, score, heard, back, back_score, ring, ring_score, came_score, near, near_score,
    s_data, r_data, s_score, r_score, s_near, r_near,
):
    hops = len(limits)
    first = limits[0]
    starts = starts_of(limits)
    pieces, firsts, _ = pieces_of(limits)
    slots = 4 * hops + 2
    me = lax.axis_index("seq")
    mate = me + 1 - 2 * (me % 2)
    onward = ways(me, devices)
    meet((*onward, mate))
    batch = 4
    bounds = [(lo, min(lo + batch, hops)) for lo in range(0, hops, batch)]
    mate_copies = []
    spans = [(4 * lo, 4 * (hi - lo)) for lo, hi in reversed(bounds)] + [(4 * hops, CAP)]
    for k, (lo, size) in enumerate(spans):
        pair = []
        for m, (src, dst) in enumerate(((y, near), (score, near_score))):
            copy = to(
                mate, src.at[pl.ds(slots + lo, size)], dst.at[pl.ds(lo, size)],
                s_near.at[m, k], r_near.at[m, k],
            )
            copy.start()
            pair.append(copy)
        mate_copies.append(pair)
    for j in range(CAP):
        back[2 * first + j] = y[4 * hops + j]
    lane = lax.broadcasted_iota(jnp.int32, score.shape[1:], 1)

    started = []
    copies = {}

    def send(t, way, q, a, b):
        dst = back.at[pl.ds(way * first + a, b - a)] if t == 1 else (
            ring.at[way, pl.ds(starts[t - 2] + a, b - a)]
        )
        number = firsts[t - 1] + q
        copy = to(
            onward[1 - way], ring.at[way, pl.ds(starts[t - 1] + a, b - a)], dst,
            s_data.at[way, number], r_data.at[way, number],
        )
        copy.start()
        started.append(copy)
        copies[t, way, q] = copy

    def send_score(t, way):
        copy = to(
            onward[1 - way], ring_score.at[way, t - 1],
            back_score.at[way] if t == 1 else came_score.at[way, t - 2],
            s_score.at[way, t - 1], r_score.at[way, t - 1],
        )
        copy.start()
        started.append(copy)
        copies[t, way, None] = copy

    for t in range(hops, 0, -1):
        if (hops - t) % batch == 0:
            for copy in mate_copies[(hops - t) // batch]:
                copy.wait_recv()
        came = limits[t] if t < hops else 0
        mine = []
        for way in (0, 1):
            entries = []
            for who, own, own_score in ((me, y, score), (mate, near, near_score)):
                for j in range(CAP):
                    slot = 4 * (t - 1) + CAP * way + j
                    entries.append((
                        heard[way, t - 1, 0, j * devices + who], own, own_score, slot
                    ))
            mine.append(entries)
        for way in (0, 1):
            if t < hops:
                copies[t + 1, way, None].wait_recv()
                tile = came_score[way, t - 1]
            else:
                tile = jnp.zeros_like(lane, jnp.float32)
            for place, _, own_score, slot in mine[way]:
                tile = jnp.where(lane == place, own_score[slot], tile)
            ring_score[way, t - 1] = tile
        came_pieces = pieces[t] if t < hops else []
        for q, (a, b) in enumerate(pieces[t - 1]):
            for way in (0, 1):
                if q < len(came_pieces):
                    copies[t + 1, way, q].wait_recv()
                middle = max(a, min(b, came))
                base = starts[t - 1]
                entries = mine[way]

                def merge(k, old):
                    for place, own, _, slot in entries:
                        old = jnp.where(place == k, own[slot], old)
                    ring[way, base + k] = old

                def over(k, _):
                    merge(k, ring[way, base + k])
                    return 0

                def fresh(k, _):
                    merge(k, entries[0][1][entries[0][3]])
                    return 0

                if middle > a:
                    lax.fori_loop(a, middle, over, 0)
                if b > middle:
                    lax.fori_loop(middle, b, fresh, 0)
                send(t, way, q, a, b)
        for way in (0, 1):
            send_score(t, way)
    for copy in mate_copies[-1]:
        copy.wait_recv()
    tile = jnp.zeros_like(lane, jnp.float32)
    for j in range(CAP):
        back[2 * first + CAP + j] = near[4 * hops + j]
        tile = jnp.where(lane == j, score[4 * hops + j], tile)
        tile = jnp.where(lane == CAP + j, near_score[4 * hops + j], tile)
    back_score[2] = tile
    for (t, _, _), copy in copies.items():
        if t == 1:
            copy.wait_recv()
    for copy in started + [copy for pair in mate_copies for copy in pair]:
        copy.wait_send()


def bring(limits, devices, y, score, heard, collective_id):
    hops = len(limits)
    slots = 4 * hops + 2
    piece_count = pieces_of(limits)[2]
    shape = y.shape[1:]
    spans = (hops - 1) // 4 + 2
    total = 2 * limits[0] + 2 * CAP
    vmem = pl.BlockSpec(memory_space=pltpu.VMEM)
    smem = pl.BlockSpec(memory_space=pltpu.SMEM)
    dma = pltpu.SemaphoreType.DMA
    return pl.pallas_call(
        functools.partial(bring_kernel, limits, devices),
        out_shape=(
            jax.ShapeDtypeStruct((total, *shape), y.dtype),
            jax.ShapeDtypeStruct((3, *score.shape[1:]), score.dtype),
        ),
        in_specs=[vmem, vmem, smem],
        out_specs=(vmem, vmem),
        scratch_shapes=[
            pltpu.VMEM((2, sum(limits), *shape), y.dtype),
            pltpu.VMEM((2, hops, *score.shape[1:]), score.dtype),
            pltpu.VMEM((2, hops, *score.shape[1:]), score.dtype),
            pltpu.VMEM((slots, *shape), y.dtype),
            pltpu.VMEM((slots, *score.shape[1:]), score.dtype),
            dma((2, piece_count)),
            dma((2, piece_count)),
            dma((2, hops)),
            dma((2, hops)),
            dma((2, spans)),
            dma((2, spans)),
        ],
        compiler_params=pltpu.CompilerParams(
            collective_id=collective_id, has_side_effects=True, vmem_limit_bytes=60 << 20
        ),
        name=f"bring{collective_id}",
    )(y, score, heard)


def normalize(rows, norm_gain):
    widened = rows.astype(jnp.float32)
    inverse_rms = lax.rsqrt(jnp.mean(widened * widened, axis=-1, keepdims=True) + norm_eps)
    return (widened * inverse_rms * norm_gain).astype(jnp.bfloat16)


def plan(target, me, devices, limits):
    count = target.shape[0]
    chips = devices // CORES
    half = chips // 2
    index = jnp.arange(count, dtype=jnp.int32)
    dist = (target // CORES - me // CORES + chips) % chips
    away = dist > 0
    order = dist * count + index
    rank = jnp.sum(((order[None, :] < order[:, None]) & away[None, :]).astype(jnp.int32), axis=1)
    total = jnp.sum(away.astype(jnp.int32))
    least = jnp.sum((away & (dist < half)).astype(jnp.int32))
    upmost = jnp.sum((away & (dist <= half)).astype(jnp.int32))
    cut = jnp.clip((total + 1 - me % CORES) // 2, least, upmost)
    up = rank < cut
    place = jnp.where(up, cut - 1 - rank, rank - cut)
    hop = jnp.where(up, dist, chips - dist)
    way = jnp.where(away, jnp.where(up, 0, 1), 2)
    room = jnp.zeros_like(place)
    for t, limit in enumerate(limits, 1):
        room = jnp.where(hop == t, limit, room)
    fits = place < room
    same = (target[None, :] == target[:, None]) & (index[None, :] < index[:, None])
    pair = jnp.sum(same.astype(jnp.int32), axis=1)
    first = limits[0]
    at_home = 2 * first + jnp.where(target == me, 0, CAP) + pair
    entry = jnp.where(away, way * first + place, at_home)
    lines = jnp.arange(2 * first + 2 * CAP, dtype=jnp.int32)
    held = (lines[:, None] == entry[None, :]) & (fits | ~away)[None, :]
    item_of = jnp.sum(jnp.where(held, index[None, :], 0), axis=1)
    lane = pair * devices + target
    lanes = jnp.arange(CAP * devices, dtype=jnp.int32)
    value = jnp.where(fits, place + 1, -1)
    notes = jnp.stack([
        jnp.sum(
            jnp.where((lanes[:, None] == lane[None, :]) & (way == w)[None, :], value[None, :], 0),
            axis=1,
        )
        for w in (0, 1)
    ]) - 1
    return entry, item_of, notes.reshape(2, 1, -1)


def shards(
    corpus,
    window_ends,
    norm_gain,
    routes,
    in_blocks,
    out_blocks,
    enc_weight,
    enc_bias,
    latent_cutoffs,
    dec_weight,
    readout,
    dec_bias,
    usual=USUAL,
):
    devices = lax.axis_size("seq")
    me = lax.axis_index("seq")
    hops = devices // CORES // 2
    model_width = corpus.shape[1]
    blocks_all = model_width // BLK
    below_rows = lax.ppermute(
        corpus[-LEN:], "seq", [(i, i + 1) for i in range(devices - 1)]
    )
    extended = jnp.concatenate([below_rows, corpus], axis=0)

    def take_one(end_offset):
        return lax.dynamic_slice_in_dim(extended, end_offset + 1, LEN, 0)

    windows = jax.vmap(take_one)(window_ends).reshape(-1, model_width)
    normal = normalize(windows, norm_gain)
    segments = normal.reshape(-1, SEG, model_width)
    seg_count = segments.shape[0]
    fanout = routes.shape[1]
    target = routes.reshape(-1)
    block_grid = segments.reshape(seg_count, SEG, blocks_all, BLK)
    enc_blocks = enc_weight.reshape(KEEP, BLK, -1)

    def out(limits, collective_id):
        entry, item_of, notes = plan(target, me, devices, limits)
        outgoing = block_grid[(item_of // fanout)[:, None], :, in_blocks[target[item_of]]]
        x, heard, heard_near = carry(limits, devices, outgoing, notes, collective_id)
        return x, heard, entry, notes, heard_near

    def home(limits, collective_id, y, score, heard, entry):
        back, back_score = bring(limits, devices, y, score, heard, collective_id)
        first = limits[0]
        column = jnp.where(
            entry < first, entry,
            jnp.where(entry < 2 * first, BLK - first + entry, 2 * BLK - 2 * first + entry),
        )
        columns = jnp.arange(3 * BLK, dtype=jnp.int32).reshape(3, 1, BLK)
        picked_score = jnp.sum(
            jnp.where(columns[None] == column[:, None, None, None], back_score[None], 0.0),
            axis=(1, 3),
        )
        return back[entry], picked_score

    limits = most(hops)
    x, heard, entry, notes, heard_near = out(usual, 0)
    crowded = jnp.minimum(
        jnp.min(heard), jnp.minimum(jnp.min(heard_near), jnp.min(notes))
    ) < -1
    x, heard, entry = lax.cond(
        crowded, lambda: out(limits, 2)[:3], lambda: (x, heard, entry)
    )
    level = (
        jnp.einsum("nqsb,qbf->nsf", x, enc_blocks, preferred_element_type=jnp.float32)
        + enc_bias
    )
    firing = jax.nn.sigmoid((level - latent_cutoffs) / step_sharpness)
    active = level * firing
    active_half = active.astype(jnp.bfloat16)
    decoded = jnp.einsum(
        "nsf,fo->nso", active_half, dec_weight, preferred_element_type=jnp.float32
    ).astype(jnp.bfloat16)
    score = jnp.sum(active * readout, axis=-1).astype(jnp.bfloat16).astype(jnp.float32)
    slope = (
        readout * (firing + level * firing * (1.0 - firing) / step_sharpness)
    ).astype(jnp.bfloat16)
    pulled = jnp.einsum(
        "nsf,qbf->nqsb", slope, enc_blocks, preferred_element_type=jnp.float32
    ).astype(jnp.bfloat16)
    decoded = decoded.reshape(-1, SEG, KEEP, BLK).transpose(0, 2, 1, 3)
    y = jnp.concatenate([decoded, pulled], axis=1)
    score = jnp.broadcast_to(score[:, :, None], (*score.shape, BLK))
    picked, picked_score = lax.cond(
        crowded,
        lambda: home(limits, 3, y, score, heard, entry),
        lambda: home(usual, 1, y, score, heard, entry),
    )
    recon_items = picked[:, :KEEP].reshape(seg_count, fanout, KEEP, SEG, BLK)
    grad_items = picked[:, KEEP:].reshape(seg_count, fanout, KEEP, SEG, BLK)
    block_ids = jnp.arange(blocks_all, dtype=jnp.int32)[None, None, :]

    def placed(blocks, values):
        where = (
            (blocks[target][:, :, None] == block_ids)
            .astype(jnp.bfloat16)
            .reshape(seg_count, fanout, KEEP, blocks_all)
        )
        return jnp.einsum(
            "tkqrb,tkqj->trjb", values, where, preferred_element_type=jnp.float32
        ).reshape(-1, model_width)

    recon_sum = placed(out_blocks, recon_items)
    grad_sum = placed(in_blocks, grad_items)
    feature_score = jnp.sum(
        picked_score.reshape(seg_count, fanout, SEG), axis=1
    ).reshape(-1)
    reconstruction = (recon_sum + dec_bias).astype(jnp.bfloat16)
    attribution = (normal.astype(jnp.float32) * grad_sum).astype(jnp.bfloat16)
    return reconstruction, attribution, feature_score


def solution(mesh):
    in_specs = (
        P(("grp", "seq"), None),
        P(("grp", "seq")),
        P(),
        P(("grp", "seq"), None),
        P(),
        P(),
        P(None, "seq"),
        P("seq"),
        P("seq"),
        P("seq", None),
        P("seq"),
        P(),
    )
    out_specs = (P(("grp", "seq"), None), P(("grp", "seq"), None), P(("grp", "seq")))
    return jax.shard_map(shards, mesh=mesh, in_specs=in_specs, out_specs=out_specs, check_vma=False)
```
